32 devices in a mesh: section: 4 (over y, core), seq: 8 (over z, x).
Axes of the slice: x: 2, y: 2, z: 4, core: 2. Of those that a mesh axis runs over, the one named last changes fastest.
Arguments:
- queries: bfloat16 [4, 64, 4096], P('section', 'seq'), may hold values from -110 to 110
- key_value_pages: bfloat16 [4, 16, 4, 2048], P('section', 'seq'), may hold values from -5 to 5
- block_table: int32 [4, 16], replicated, may hold values from 0 to 15, as said below
- page_mask: int32 [4, 64], replicated, may hold values from 0 to 1, as said below
- noise_level: int32 [4], replicated, may hold values from 0 to 15
- level_gate: float32 [16, 4096], replicated, may hold values from 0.5 to 1.5
Outputs:
- attended: bfloat16 [4, 64, 4096], P('section', 'seq')
The draws below stay inside these ranges and needn't reach their ends.
Inputs may be any that keep to these rules, and one draw needn't show every extreme that they name: `block_table`: each row is a permutation of 0 to 15. `page_mask`: a query span sees all pages of its own span, none of later spans, and some pages of earlier spans.
All inputs are finite; a program needn't handle non-finite values.
Results may differ from the reference program's by a relative error of at most 0.0065.
Values may be sent and summed in bfloat16 or wider, within the bound.
No kernel may reach another device: no remote copies, remote signals or barrier semaphores. Data moves between devices by JAX's collectives and lax.ppermute only.
A program may use at most 64 MiB of HBM per device.

```python
import jax
import jax.numpy as jnp
from jax import lax

QUERY_HEADS = 32
KEY_VALUE_HEADS = 8
HEAD_WIDTH = 128
PAGE_TOKENS = 4
LEVELS = 16
VIDEO_SPANS = 4
SPAN_TOKENS = 64
SPAN_PAGES = 16


def shared_pool(key):
    key_value_pool = jax.random.normal(jax.random.fold_in(key, 7), (VIDEO_SPANS, SPAN_PAGES, PAGE_TOKENS, 2 * KEY_VALUE_HEADS * HEAD_WIDTH), jnp.float32)
    key_value_pool = jnp.clip(key_value_pool, -5.0, 5.0)
    return key_value_pool


def shared_tables(key):
    base = jax.random.fold_in(key, 3)
    table = jax.vmap(lambda span: jax.random.permutation(jax.random.fold_in(base, span), SPAN_PAGES))(jnp.arange(VIDEO_SPANS))
    table = table.astype(jnp.int32)
    keep = jax.random.randint(jax.random.fold_in(key, 4), (VIDEO_SPANS, VIDEO_SPANS, SPAN_PAGES), 0, 4) > 0
    query_row = jnp.arange(VIDEO_SPANS)[:, None, None]
    key_span = jnp.arange(VIDEO_SPANS)[None, :, None]
    mask_full = jnp.where(key_span < query_row, keep, key_span == query_row)
    forced = (key_span == 0) & (table[0][None, None, :] <= 1)
    mask_full = (mask_full | forced).astype(jnp.int32).reshape(VIDEO_SPANS, VIDEO_SPANS * SPAN_PAGES)
    return (table, mask_full)


def draw_key_value_pages(key, part):
    return shared_pool(key).astype(jnp.bfloat16)


def draw_block_table(key, part):
    return shared_tables(key)[0]


def draw_page_mask(key, part):
    return shared_tables(key)[1]


def draw_queries(key, part):
    value_rows = jax.random.normal(jax.random.fold_in(key, 5), (VIDEO_SPANS, SPAN_TOKENS, QUERY_HEADS * HEAD_WIDTH), jnp.float32)
    value_rows = jnp.clip(value_rows, -5.0, 5.0)
    value_rows = jnp.clip(value_rows, -110.0, 110.0)
    return value_rows.astype(jnp.bfloat16)


def touch_ends(values, stream_key, smallest, largest):
    shape = values.shape
    spot = [jax.random.randint(jax.random.fold_in(stream_key, axis), (), 0, shape[axis]) for axis in range(len(shape))]
    values = values.at[tuple(spot)].set(smallest)
    longest = shape.index(max(shape))
    spot[longest] = (spot[longest] + 1) % shape[longest]
    return values.at[tuple(spot)].set(largest)


def setup_inputs(seed: int = 0) -> dict:
    streams_of = jax.random.split(jax.random.key(seed), 7)
    queries = draw_queries(jax.random.fold_in(streams_of[6], 71), 0)
    key_value_pages = draw_key_value_pages(jax.random.fold_in(streams_of[6], 71), 0)
    block_table = draw_block_table(jax.random.fold_in(streams_of[6], 71), 0)
    page_mask = draw_page_mask(jax.random.fold_in(streams_of[6], 71), 0)
    noise_level = touch_ends(jax.random.randint(streams_of[4], (VIDEO_SPANS,), 0, LEVELS), jax.random.fold_in(streams_of[4], 1), 0, LEVELS - 1).astype(jnp.int32)
    level_gate = jnp.clip(jax.random.uniform(streams_of[5], (LEVELS, QUERY_HEADS * HEAD_WIDTH), jnp.float32, 0.5, 1.5), 0.5, 1.5)
    return {"queries": queries, "key_value_pages": key_value_pages, "block_table": block_table, "page_mask": page_mask, "noise_level": noise_level, "level_gate": level_gate}


eps = 1e-06

def reference(queries, key_value_pages, block_table, page_mask, noise_level, level_gate):
    span_group = QUERY_HEADS // KEY_VALUE_HEADS
    onehot = (block_table[:, :, None] == jnp.arange(SPAN_PAGES, dtype=jnp.int32)[None, None, :]).astype(jnp.float32)
    logical = page_mask.reshape(VIDEO_SPANS, VIDEO_SPANS, SPAN_PAGES).astype(jnp.float32)
    visible = jnp.einsum('qci,cip->qcp', logical, onehot)
    token_visible = jnp.repeat(visible, PAGE_TOKENS, axis=2).reshape(VIDEO_SPANS, VIDEO_SPANS * SPAN_TOKENS) > 0.5
    gathered_keys = key_value_pages[:, :, :, :KEY_VALUE_HEADS * HEAD_WIDTH].reshape(VIDEO_SPANS * SPAN_TOKENS, KEY_VALUE_HEADS, HEAD_WIDTH)
    gathered_values = key_value_pages[:, :, :, KEY_VALUE_HEADS * HEAD_WIDTH:].reshape(VIDEO_SPANS * SPAN_TOKENS, KEY_VALUE_HEADS, HEAD_WIDTH)
    levels = (noise_level[:, None] == jnp.arange(LEVELS, dtype=jnp.int32)[None, :]).astype(jnp.float32)
    gates = jnp.dot(levels, level_gate, precision=lax.Precision.HIGHEST).reshape(VIDEO_SPANS, QUERY_HEADS, HEAD_WIDTH)
    scale = HEAD_WIDTH ** (-0.5)

    def one_span(span):
        rows = lax.dynamic_index_in_dim(queries, span, 0, keepdims=False).reshape(SPAN_TOKENS, QUERY_HEADS, HEAD_WIDTH)
        seen = lax.dynamic_index_in_dim(token_visible, span, 0, keepdims=False)

        def one_head(head):
            query = lax.dynamic_index_in_dim(rows, head, 1, keepdims=False)
            keys = lax.dynamic_index_in_dim(gathered_keys, head // span_group, 1, keepdims=False)
            value_rows = lax.dynamic_index_in_dim(gathered_values, head // span_group, 1, keepdims=False)
            scores = jnp.dot(query, keys.T, preferred_element_type=jnp.float32) * scale
            scores = jnp.where(seen[None, :], scores, -1e+30)
            top = lax.optimization_barrier(jnp.max(scores, axis=-1, keepdims=True))
            weights = jnp.where(seen[None, :], jnp.exp(scores - top), 0.0)
            total = lax.optimization_barrier(jnp.sum(weights, axis=-1, keepdims=True))
            return jnp.dot(weights.astype(jnp.bfloat16), value_rows, preferred_element_type=jnp.float32) / total
        heads = lax.map(one_head, jnp.arange(QUERY_HEADS, dtype=jnp.int32))
        heads = jnp.transpose(heads, (1, 0, 2))
        normed = heads * lax.rsqrt(lax.optimization_barrier(jnp.mean(heads * heads, axis=-1, keepdims=True)) + eps)
        gate = lax.dynamic_index_in_dim(gates, span, 0, keepdims=False)
        return (normed * gate[None, :, :]).astype(jnp.bfloat16).reshape(SPAN_TOKENS, QUERY_HEADS * HEAD_WIDTH)
    return lax.map(one_span, jnp.arange(VIDEO_SPANS, dtype=jnp.int32))
```

```python
import functools
import math

import jax
import jax.numpy as jnp
from jax import lax
from jax.experimental import pallas as pl
from jax.experimental.pallas import tpu as pltpu
from jax.sharding import PartitionSpec as P

QUERY_HEADS = 32
KEY_VALUE_HEADS = 8
HEAD_WIDTH = 128
GROUP = QUERY_HEADS // KEY_VALUE_HEADS
KEY_WIDTH = KEY_VALUE_HEADS * HEAD_WIDTH
EPS = 1e-06
HIDDEN = -1e30


BOTH = ("section", "seq")
VMEM = pl.BlockSpec(memory_space=pltpu.VMEM)
SMEM = pl.BlockSpec(memory_space=pltpu.SMEM)


def log2(size):
    bits = size.bit_length() - 1
    assert 1 << bits == size
    return bits


def column_kernel(*refs):
    *chunks, out = refs
    rows = chunks[0].shape[1] * chunks[0].shape[2]
    for index, chunk in enumerate(chunks):
        tokens = chunk[0].astype(jnp.float32).reshape(rows, chunk.shape[3])
        out[index * rows : (index + 1) * rows, :] = tokens.astype(out.dtype)


def tables_kernel(table, mask, level, gates, bias, gate, *, chunk_tokens, page_length, columns):
    section = lax.axis_index("section")
    seq = lax.axis_index("seq")
    seq_bits = log2(columns * 2)
    spans, pages = table.shape
    lane = lax.broadcasted_iota(jnp.int32, bias.shape, 1)
    chunk = lane >> log2(chunk_tokens)
    column = chunk & (columns - 1)
    piece = chunk >> log2(columns)
    core = piece & 1
    side = piece >> 1
    span = section ^ (((side >> 1) << 1) | core)
    place = seq ^ ((column << 1) | (side & 1))
    page = place * (chunk_tokens // page_length) + ((lane & (chunk_tokens - 1)) >> log2(page_length))
    key = span * pages + page

    def one_span(other, seen):
        for index in range(pages):
            hit = key == other * pages + table[other, index]
            seen = jnp.where(hit, mask[section, other * pages + index], seen)
        return seen

    seen = lax.fori_loop(0, spans, one_span, jnp.zeros(bias.shape, jnp.int32), unroll=spans <= 4)
    bias[...] = jnp.where(seen > 0, 0.0, HIDDEN).astype(jnp.float32)
    gate[...] = gates[pl.ds(level[section], 1), :]


def attend_kernel(queries, bias, gate, *refs):
    *pieces, out = refs
    tokens = queries.shape[1]
    scale = HEAD_WIDTH ** (-0.5) * math.log2(math.e)
    hidden = bias[...]
    for head in range(KEY_VALUE_HEADS):
        query = jnp.concatenate(
            [
                queries[0, :, n * HEAD_WIDTH : (n + 1) * HEAD_WIDTH]
                for n in range(head * GROUP, (head + 1) * GROUP)
            ],
            axis=0,
        )
        at = head * HEAD_WIDTH
        keys = jnp.concatenate([p[:, at : at + HEAD_WIDTH] for p in pieces], axis=0)
        values = jnp.concatenate(
            [p[:, KEY_WIDTH + at : KEY_WIDTH + at + HEAD_WIDTH] for p in pieces], axis=0
        )
        scores = lax.dot_general(
            query, keys, (((1,), (1,)), ((), ())), preferred_element_type=jnp.float32
        )
        scores = scores * scale + hidden
        weights = jnp.exp2(scores - jnp.max(scores, axis=-1, keepdims=True))
        total = jnp.sum(weights, axis=-1, keepdims=True)
        mixed = jnp.dot(weights.astype(jnp.bfloat16), values, preferred_element_type=jnp.float32)
        square = jnp.mean(mixed * mixed, axis=-1, keepdims=True)
        normed = mixed * lax.rsqrt(square + EPS * (total * total))
        for g in range(GROUP):
            at = (head * GROUP + g) * HEAD_WIDTH
            rows = normed[g * tokens : (g + 1) * tokens, :] * gate[:, at : at + HEAD_WIDTH]
            out[0, :, at : at + HEAD_WIDTH] = rows.astype(out.dtype)


def body(queries, key_value_pages, block_table, page_mask, noise_level, level_gate):
    sections = lax.axis_size("section")
    places = lax.axis_size("seq")
    columns = places // 2
    devices = sections * places
    _, local_pages, page_length, width = key_value_pages.shape
    chunk_tokens = local_pages * page_length
    key_count = devices * chunk_tokens

    def swap(array, section_bits, seq_bits):
        flip = section_bits * places + seq_bits
        return lax.ppermute(array, BOTH, [(i, i ^ flip) for i in range(devices)])

    bias, gate = pl.pallas_call(
        functools.partial(
            tables_kernel, chunk_tokens=chunk_tokens, page_length=page_length, columns=columns
        ),
        out_shape=(
            jax.ShapeDtypeStruct((1, key_count), jnp.float32),
            jax.ShapeDtypeStruct((1, level_gate.shape[1]), jnp.float32),
        ),
        in_specs=[SMEM, SMEM, SMEM, VMEM],
        out_specs=(VMEM, VMEM),
        name="tables",
    )(block_table, page_mask, noise_level, level_gate)

    chunks = [key_value_pages] + [swap(key_value_pages, 0, z << 1) for z in range(1, columns)]
    column = pl.pallas_call(
        column_kernel,
        out_shape=jax.ShapeDtypeStruct((columns * chunk_tokens, width), key_value_pages.dtype),
        in_specs=[VMEM] * columns,
        out_specs=VMEM,
        name="column",
    )(*chunks)

    pieces = []
    for side in range(sections):
        near = swap(column, (side >> 1) << 1, side & 1) if side else column
        pieces += [near, swap(near, 1, 0)]

    return pl.pallas_call(
        attend_kernel,
        out_shape=jax.ShapeDtypeStruct(queries.shape, queries.dtype),
        in_specs=[VMEM] * (3 + len(pieces)),
        out_specs=VMEM,
        name="attend",
    )(queries, bias, gate, *pieces)


def solution(mesh):
    return jax.shard_map(
        body,
        mesh=mesh,
        in_specs=(P("section", "seq", None), P("section", "seq", None, None), P(), P(), P(), P()),
        out_specs=P("section", "seq", None),
        check_vma=False,
    )
```

```python
import functools
import math

import jax
import jax.numpy as jnp
from jax import lax
from jax.experimental import pallas as pl
from jax.experimental.pallas import tpu as pltpu
from jax.sharding import PartitionSpec as P

QUERY_HEADS = 32
KEY_VALUE_HEADS = 8
HEAD_WIDTH = 128
GROUP = QUERY_HEADS // KEY_VALUE_HEADS
KEY_WIDTH = KEY_VALUE_HEADS * HEAD_WIDTH
EPS = 1e-06
HIDDEN = -1e30


BOTH = ("section", "seq")
VMEM = pl.BlockSpec(memory_space=pltpu.VMEM)
SMEM = pl.BlockSpec(memory_space=pltpu.SMEM)


def grant(*arrays):
    held = sum(a.size * a.dtype.itemsize for a in arrays)
    return pltpu.CompilerParams(vmem_limit_bytes=(4 << 20) + 2 * held)


def log2(size):
    bits = size.bit_length() - 1
    assert 1 << bits == size
    return bits


def column_kernel(*refs):
    *chunks, _, out = refs
    rows = chunks[0].shape[1] * chunks[0].shape[2]
    for index, chunk in enumerate(chunks):
        tokens = chunk[0].astype(jnp.float32).reshape(rows, chunk.shape[3])
        out[index * rows : (index + 1) * rows, :] = tokens.astype(out.dtype)


def tables_kernel(table, mask, level, gates, bias, gate, *, chunk_tokens, page_length, columns):
    section = lax.axis_index("section")
    seq = lax.axis_index("seq")
    seq_bits = log2(columns * 2)
    spans, pages = table.shape
    lane = lax.broadcasted_iota(jnp.int32, bias.shape, 1)
    chunk = lane >> log2(chunk_tokens)
    column = chunk & (columns - 1)
    piece = chunk >> log2(columns)
    core = piece & 1
    side = piece >> 1
    span = section ^ (((side >> 1) << 1) | core)
    place = seq ^ ((column << 1) | (side & 1))
    page = place * (chunk_tokens // page_length) + ((lane & (chunk_tokens - 1)) >> log2(page_length))
    key = span * pages + page

    def one_span(other, seen):
        for index in range(pages):
            hit = key == other * pages + table[other, index]
            seen = jnp.where(hit, mask[section, other * pages + index], seen)
        return seen

    seen = lax.fori_loop(0, spans, one_span, jnp.zeros(bias.shape, jnp.int32), unroll=spans <= 4)
    bias[...] = jnp.where(seen > 0, 0.0, HIDDEN).astype(jnp.float32)
    gate[...] = gates[pl.ds(level[section], 1), :]


def attend_kernel(queries, bias, gate, *refs):
    *pieces, out = refs
    tokens = queries.shape[1]
    scale = HEAD_WIDTH ** (-0.5) * math.log2(math.e)
    hidden = bias[...]
    for head in range(KEY_VALUE_HEADS):
        query = jnp.concatenate(
            [
                queries[0, :, n * HEAD_WIDTH : (n + 1) * HEAD_WIDTH]
                for n in range(head * GROUP, (head + 1) * GROUP)
            ],
            axis=0,
        )
        at = head * HEAD_WIDTH
        keys = jnp.concatenate([p[:, at : at + HEAD_WIDTH] for p in pieces], axis=0)
        values = jnp.concatenate(
            [p[:, KEY_WIDTH + at : KEY_WIDTH + at + HEAD_WIDTH] for p in pieces], axis=0
        )
        scores = lax.dot_general(
            query, keys, (((1,), (1,)), ((), ())), preferred_element_type=jnp.float32
        )
        scores = scores * scale + hidden
        weights = jnp.exp2(scores - jnp.max(scores, axis=-1, keepdims=True))
        total = jnp.sum(weights, axis=-1, keepdims=True)
        mixed = jnp.dot(weights.astype(jnp.bfloat16), values, preferred_element_type=jnp.float32)
        square = jnp.mean(mixed * mixed, axis=-1, keepdims=True)
        normed = mixed * lax.rsqrt(square + EPS * (total * total))
        for g in range(GROUP):
            at = (head * GROUP + g) * HEAD_WIDTH
            rows = normed[g * tokens : (g + 1) * tokens, :] * gate[:, at : at + HEAD_WIDTH]
            out[0, :, at : at + HEAD_WIDTH] = rows.astype(out.dtype)


def body(queries, key_value_pages, block_table, page_mask, noise_level, level_gate):
    sections = lax.axis_size("section")
    places = lax.axis_size("seq")
    columns = places // 2
    devices = sections * places
    _, local_pages, page_length, width = key_value_pages.shape
    chunk_tokens = local_pages * page_length
    key_count = devices * chunk_tokens

    def swap(array, section_bits, seq_bits):
        flip = section_bits * places + seq_bits
        return lax.ppermute(array, BOTH, [(i, i ^ flip) for i in range(devices)])

    bias, gate = pl.pallas_call(
        functools.partial(
            tables_kernel, chunk_tokens=chunk_tokens, page_length=page_length, columns=columns
        ),
        out_shape=(
            jax.ShapeDtypeStruct((1, key_count), jnp.float32),
            jax.ShapeDtypeStruct((1, level_gate.shape[1]), jnp.float32),
        ),
        in_specs=[SMEM, SMEM, SMEM, VMEM],
        out_specs=(VMEM, VMEM),
        compiler_params=grant(level_gate),
        name="tables",
    )(block_table, page_mask, noise_level, level_gate)

    chunks = [key_value_pages] + [swap(key_value_pages, 0, z << 1) for z in range(1, columns)]
    column = pl.pallas_call(
        column_kernel,
        out_shape=jax.ShapeDtypeStruct((columns * chunk_tokens, width), key_value_pages.dtype),
        in_specs=[VMEM] * columns + [pl.BlockSpec(memory_space=pl.ANY)],
        out_specs=VMEM,
        compiler_params=grant(*chunks),
        name="column",
    )(*chunks, bias)

    pieces = []
    for side in range(sections):
        near = swap(column, (side >> 1) << 1, side & 1) if side else column
        pieces += [near, swap(near, 1, 0)]

    return pl.pallas_call(
        attend_kernel,
        out_shape=jax.ShapeDtypeStruct(queries.shape, queries.dtype),
        in_specs=[VMEM] * (3 + len(pieces)),
        out_specs=VMEM,
        compiler_params=grant(*pieces),
        name="attend",
    )(queries, bias, gate, *pieces)


def solution(mesh):
    return jax.shard_map(
        body,
        mesh=mesh,
        in_specs=(P("section", "seq", None), P("section", "seq", None, None), P(), P(), P(), P()),
        out_specs=P("section", "seq", None),
        check_vma=False,
    )
```

```python
import functools
import math

import jax
import jax.numpy as jnp
from jax import lax
from jax.experimental import pallas as pl
from jax.experimental.pallas import tpu as pltpu
from jax.sharding import PartitionSpec as P


QUERY_HEADS = 32
KEY_VALUE_HEADS = 8
HEAD_WIDTH = 128
GROUP = QUERY_HEADS // KEY_VALUE_HEADS
KEY_WIDTH = KEY_VALUE_HEADS * HEAD_WIDTH
EPS = 1e-06
HIDDEN = -1e30


BOTH = ("section", "seq")
VMEM = pl.BlockSpec(memory_space=pltpu.VMEM)
SMEM = pl.BlockSpec(memory_space=pltpu.SMEM)


def grant(*arrays):
    held = sum(a.size * a.dtype.itemsize for a in arrays)
    return pltpu.CompilerParams(vmem_limit_bytes=(4 << 20) + 2 * held)


def log2(size):
    bits = size.bit_length() - 1
    assert 1 << bits == size
    return bits


def column_kernel(*refs):
    *chunks, _, out = refs
    rows = chunks[0].shape[1] * chunks[0].shape[2]
    for index, chunk in enumerate(chunks):
        tokens = chunk[0].astype(jnp.float32).reshape(rows, chunk.shape[3])
        out[index * rows : (index + 1) * rows, :] = tokens.astype(out.dtype)


def tables_kernel(table, mask, level, gates, bias, gate, *, chunk_tokens, page_length, columns):
    section = lax.axis_index("section")
    seq = lax.axis_index("seq")
    spans, pages = table.shape
    lane = lax.broadcasted_iota(jnp.int32, bias.shape, 1)
    chunk = lane >> log2(chunk_tokens)
    column = chunk & (columns - 1)
    piece = chunk >> log2(columns)
    core = piece & 1
    side = piece >> 1
    span = section ^ (((side >> 1) << 1) | core)
    place = seq ^ ((column << 1) | (side & 1))
    page = place * (chunk_tokens // page_length) + ((lane & (chunk_tokens - 1)) >> log2(page_length))
    key = span * pages + page

    def one_span(other, seen):
        for index in range(pages):
            hit = key == other * pages + table[other, index]
            seen = jnp.where(hit, mask[section, other * pages + index], seen)
        return seen

    seen = lax.fori_loop(0, spans, one_span, jnp.zeros(bias.shape, jnp.int32), unroll=spans <= 4)
    bias[...] = jnp.where(seen > 0, 0.0, HIDDEN).astype(jnp.float32)
    gate[...] = gates[pl.ds(level[section], 1), :]


def attend_kernel(queries, bias, gate, *refs):
    *pieces, out = refs
    tokens = queries.shape[1]
    scale = HEAD_WIDTH ** (-0.5) * math.log2(math.e)
    hidden = bias[...]
    heads = range(KEY_VALUE_HEADS)
    scores = []
    for head in heads:
        query = jnp.concatenate(
            [
                queries[0, :, n * HEAD_WIDTH : (n + 1) * HEAD_WIDTH]
                for n in range(head * GROUP, (head + 1) * GROUP)
            ],
            axis=0,
        )
        at = head * HEAD_WIDTH
        keys = jnp.concatenate([p[:, at : at + HEAD_WIDTH] for p in pieces], axis=0)
        scores.append(
            lax.dot_general(query, keys, (((1,), (1,)), ((), ())), preferred_element_type=jnp.float32)
        )
    scores = jnp.concatenate(scores, axis=0) * scale + hidden
    weights = jnp.exp2(scores - jnp.max(scores, axis=-1, keepdims=True))
    total = jnp.sum(weights, axis=-1, keepdims=True)
    weights = weights.astype(jnp.bfloat16)
    rows = tokens * GROUP
    mixed = []
    for head in heads:
        at = KEY_WIDTH + head * HEAD_WIDTH
        values = jnp.concatenate([p[:, at : at + HEAD_WIDTH] for p in pieces], axis=0)
        mixed.append(
            jnp.dot(
                weights[head * rows : (head + 1) * rows], values, preferred_element_type=jnp.float32
            )
        )
    mixed = jnp.concatenate(mixed, axis=0)
    square = jnp.mean(mixed * mixed, axis=-1, keepdims=True)
    normed = mixed * lax.rsqrt(square + EPS * (total * total))
    for n in range(QUERY_HEADS):
        at = n * HEAD_WIDTH
        part = normed[n * tokens : (n + 1) * tokens, :] * gate[:, at : at + HEAD_WIDTH]
        out[0, :, at : at + HEAD_WIDTH] = part.astype(out.dtype)


def body(queries, key_value_pages, block_table, page_mask, noise_level, level_gate):
    sections = lax.axis_size("section")
    places = lax.axis_size("seq")
    columns = places // 2
    devices = sections * places
    _, local_pages, page_length, width = key_value_pages.shape
    chunk_tokens = local_pages * page_length
    key_count = devices * chunk_tokens

    def swap(array, section_bits, seq_bits):
        flip = section_bits * places + seq_bits
        return lax.ppermute(array, BOTH, [(i, i ^ flip) for i in range(devices)])

    bias, gate = pl.pallas_call(
        functools.partial(
            tables_kernel, chunk_tokens=chunk_tokens, page_length=page_length, columns=columns
        ),
        out_shape=(
            jax.ShapeDtypeStruct((1, key_count), jnp.float32),
            jax.ShapeDtypeStruct((1, level_gate.shape[1]), jnp.float32),
        ),
        in_specs=[SMEM, SMEM, SMEM, VMEM],
        out_specs=(VMEM, VMEM),
        compiler_params=grant(level_gate),
        name="tables",
    )(block_table, page_mask, noise_level, level_gate)

    chunks = [key_value_pages] + [swap(key_value_pages, 0, z << 1) for z in range(1, columns)]
    column = pl.pallas_call(
        column_kernel,
        out_shape=jax.ShapeDtypeStruct((columns * chunk_tokens, width), key_value_pages.dtype),
        in_specs=[VMEM] * columns + [pl.BlockSpec(memory_space=pl.ANY)],
        out_specs=VMEM,
        compiler_params=grant(*chunks),
        name="column",
    )(*chunks, bias)

    pieces = []
    for side in range(sections):
        near = column
        if side:
            near = swap(column, (side >> 1) << 1, side & 1)
        pieces += [near, swap(near, 1, 0)]

    return pl.pallas_call(
        attend_kernel,
        out_shape=jax.ShapeDtypeStruct(queries.shape, queries.dtype),
        in_specs=[VMEM] * (3 + len(pieces)),
        out_specs=VMEM,
        compiler_params=grant(*pieces),
        name="attend",
    )(queries, bias, gate, *pieces)


def solution(mesh):
    return jax.shard_map(
        body,
        mesh=mesh,
        in_specs=(P("section", "seq", None), P("section", "seq", None, None), P(), P(), P(), P()),
        out_specs=P("section", "seq", None),
        check_vma=False,
    )
```
